32 devices in a mesh: row: 4 (over y, x), col: 8 (over z, core).
Axes of the slice: x: 2, y: 2, z: 4, core: 2. Of those that a mesh axis runs over, the one named last changes fastest.
Arguments:
- tile_data: bfloat16 [128, 128, 128], P(('row', 'col')), may hold values from -24 to 24
- tile_coords: int32 [3, 128], P(None, ('row', 'col')), may hold values from 0 to 255, as said below
- tile_counts: int32 [32], P(('row', 'col')), may hold values from 1 to 4, as said below
- factor_rows: float32 [64, 8192], P(None, ('row', 'col')), may hold values from -6 to 6
- factor_cols: float32 [64, 16384], P(None, ('col', 'row')), may hold values from -6 to 6
- factor_depth: float32 [64, 256], P(None, ('row', 'col')), may hold values from -6 to 6
- damping: float32 [], replicated, may hold values from 64 to 256
Outputs:
- step_a: float32 [64, 8192], P(None, ('row', 'col'))
- step_b: float32 [64, 16384], P(None, ('col', 'row'))
- step_c: float32 [64, 256], P(None, ('row', 'col'))
The draws below stay inside these ranges and needn't reach their ends.
Inputs may be any that keep to these rules, and one draw needn't show every extreme that they name: `tile_coords`: the first row names a tile's block within its device's group of 16 first-mode blocks, the second its block within the group of 16 second-mode blocks, the third its third-mode index below 256. `tile_counts`: slots at and beyond a device's count are padding and carry nothing; some device fills all 4 slots.
All inputs are finite; a program needn't handle non-finite values.
Results may differ from the reference program's by a relative error of at most 0.0003.
Values sent between devices are 32-bit elements; how exact they have to be, the bound alone decides.
A program may use at most 64 MiB of HBM per device.

```python
import math
import jax
import jax.numpy as jnp
from jax import lax

RANK = 64
TILE = 128
RB = 16
CB = 16
TCAP = 4
ITERS = 2
MODE_ROWS = 8192
MODE_COLS = 16384
DEPTH = 256
TILES_ALL = 128
N_ROW = 4
N_COL = 8


def draw_tile_coords(key, part):
    key_rows, key_cols, key_depth = jax.random.split(key, 3)
    block_rows = jax.random.randint(key_rows, (TILES_ALL,), 0, RB)
    block_cols = jax.random.randint(key_cols, (TILES_ALL,), 0, CB)
    depth_index = jax.random.randint(key_depth, (TILES_ALL,), 0, DEPTH)
    return jnp.stack([block_rows, block_cols, depth_index]).astype(jnp.int32)


def draw_tile_counts(key, part):
    key_base, key_top = jax.random.split(key, 2)
    device_total = N_ROW * N_COL
    base_counts = jax.random.randint(key_base, (device_total,), TCAP // 4, TCAP + 1)
    fullest = jax.random.randint(key_top, (), 0, device_total)
    placed = jnp.arange(device_total, dtype=jnp.int32) == fullest
    return jnp.where(placed, TCAP, base_counts).astype(jnp.int32)


def level_of(stream_key, shape, cuts, least, largest):
    loudness, own = 1.0, jax.random.fold_in(stream_key, 6)
    for position, shards_of in cuts:
        heights = jnp.exp(jax.random.uniform(jax.random.fold_in(own, position), (shards_of,), jnp.float32, least / len(cuts), largest / len(cuts)))
        loudness = loudness * jnp.repeat(heights, shape[position] // shards_of).reshape([-1 if axis == position else 1 for axis in range(len(shape))])
    return loudness


def noise(stream_key, shape, spread, most, cuts=(), kind=jnp.bfloat16):
    factor_of = level_of(stream_key, shape, cuts, -0.22, 0.18) if cuts else 1.0
    result = jax.random.normal(stream_key, shape, jnp.float32) * spread * factor_of
    return jnp.minimum(jnp.maximum(result, -most), most).astype(kind)


def setup_inputs(seed: int = 0) -> dict:
    arg_keys = jax.random.split(jax.random.key(seed), 8)
    tile_data = noise(arg_keys[0], (TILES_ALL, TILE, TILE), 4.0, 24.0, ((0, 32),))
    tile_coords = draw_tile_coords(jax.random.fold_in(arg_keys[7], 71), 0)
    tile_counts = draw_tile_counts(jax.random.fold_in(arg_keys[7], 71), 0)
    factor_rows = noise(arg_keys[3], (RANK, MODE_ROWS), 1.0, 6.0, ((1, 32),), jnp.float32)
    factor_cols = noise(arg_keys[4], (RANK, MODE_COLS), 1.0, 6.0, ((1, 32),), jnp.float32)
    factor_depth = noise(arg_keys[5], (RANK, DEPTH), 1.0, 6.0, ((1, 32),), jnp.float32)
    damping = jnp.clip(jnp.exp(jax.random.uniform(arg_keys[6], (), jnp.float32, math.log(64.0), math.log(256.0))), 64.0, 256.0)
    return {"tile_data": tile_data, "tile_coords": tile_coords, "tile_counts": tile_counts, "factor_rows": factor_rows, "factor_cols": factor_cols, "factor_depth": factor_depth, "damping": damping}


exact_precision = lax.Precision.HIGHEST


def make_onehot(indices, block_count):
    return (indices[:, None] == jnp.arange(block_count, dtype=jnp.int32)[None, :]).astype(jnp.float32)


def pick_rows(onehot, blocks):
    shaped = blocks.reshape(blocks.shape[0], onehot.shape[1], blocks.shape[1] // onehot.shape[1])
    return jnp.einsum('tq,rqa->tra', onehot.astype(blocks.dtype), shaped, precision=exact_precision)


def fold_rows(onehot, grads):
    summed = jnp.einsum('tq,tra->rqa', onehot.astype(grads.dtype), grads, precision=exact_precision)
    return summed.reshape(summed.shape[0], summed.shape[1] * summed.shape[2])


def tile_model(rows_a, rows_b, rows_c):
    return jnp.einsum('tra,trb->tab', rows_a, rows_b * rows_c[:, :, None], precision=exact_precision)


def tile_products(rows_a, rows_b, rows_c, dir_a, dir_b, dir_c):
    depth_cols = rows_c[:, :, None]
    left_side = jnp.concatenate([dir_a, rows_a, rows_a], axis=1)
    right_side = jnp.concatenate([rows_b * depth_cols, dir_b * depth_cols, rows_b * dir_c[:, :, None]], axis=1)
    return jnp.einsum('tra,trb->tab', left_side, right_side, precision=exact_precision)


def tile_transpose(values, rows_a, rows_b, rows_c):
    depth_cols = rows_c[:, :, None]
    row_raw = jnp.einsum('tab,trb->tra', values, rows_b, precision=exact_precision)
    grad_rows = row_raw * depth_cols
    grad_cols = jnp.einsum('tab,tra->trb', values, rows_a * depth_cols, precision=exact_precision)
    grad_depth = jnp.sum(rows_a * row_raw, axis=2)
    return grad_rows, grad_cols, grad_depth


def reference(tile_data, tile_coords, tile_counts, factor_rows, factor_cols, factor_depth, damping):
    rows_group = RB * TILE
    cols_group = CB * TILE

    def apply_all(direction):
        def per_device(device, totals):
            device = jnp.asarray(device).astype(jnp.int32)
            grid_row = device // N_COL
            grid_col = device % N_COL
            start_a = (grid_row * rows_group).astype(jnp.int32)
            start_b = (grid_col * cols_group).astype(jnp.int32)
            block_a = lax.dynamic_slice_in_dim(factor_rows, start_a, rows_group, 1)
            block_b = lax.dynamic_slice_in_dim(factor_cols, start_b, cols_group, 1)
            coords_here = lax.dynamic_slice_in_dim(tile_coords, (device * TCAP).astype(jnp.int32), TCAP, 1)
            live_mask = (jnp.arange(TCAP, dtype=jnp.int32) < tile_counts[device]).astype(factor_rows.dtype)[:, None, None]
            pick_a = make_onehot(coords_here[0], RB)
            pick_b = make_onehot(coords_here[1], CB)
            rows_a = pick_rows(pick_a, block_a)
            rows_b = pick_rows(pick_b, block_b)
            rows_c = jnp.take(factor_depth, coords_here[2], axis=1).T
            if direction is None:
                data_here = lax.dynamic_slice_in_dim(tile_data, (device * TCAP).astype(jnp.int32), TCAP, 0).astype(factor_rows.dtype)
                values = data_here - tile_model(rows_a, rows_b, rows_c)
            else:
                dir_block_a = lax.dynamic_slice_in_dim(direction[0], start_a, rows_group, 1)
                dir_block_b = lax.dynamic_slice_in_dim(direction[1], start_b, cols_group, 1)
                dir_c = jnp.take(direction[2], coords_here[2], axis=1).T
                values = tile_products(rows_a, rows_b, rows_c, pick_rows(pick_a, dir_block_a), pick_rows(pick_b, dir_block_b), dir_c)
            grad_rows, grad_cols, grad_depth = tile_transpose(values * live_mask, rows_a, rows_b, rows_c)
            old_a = lax.dynamic_slice_in_dim(totals[0], start_a, rows_group, 1)
            total_a = lax.dynamic_update_slice_in_dim(totals[0], old_a + fold_rows(pick_a, grad_rows), start_a, 1)
            old_b = lax.dynamic_slice_in_dim(totals[1], start_b, cols_group, 1)
            total_b = lax.dynamic_update_slice_in_dim(totals[1], old_b + fold_rows(pick_b, grad_cols), start_b, 1)
            total_c = totals[2] + jax.ops.segment_sum(grad_depth, coords_here[2], num_segments=DEPTH).T
            return (total_a, total_b, total_c)

        start = (jnp.zeros_like(factor_rows), jnp.zeros_like(factor_cols), jnp.zeros_like(factor_depth))
        return lax.fori_loop(0, N_ROW * N_COL, per_device, start)

    def hessian(direction):
        applied = apply_all(direction)
        return tuple(part_one + damping * part_two for part_one, part_two in zip(applied, direction))

    def inner(first, second):
        return sum(jnp.sum(part_one * part_two) for part_one, part_two in zip(first, second))

    rhs = apply_all(None)
    solution = tuple(jnp.zeros_like(member) for member in rhs)
    residual = rhs
    direction = rhs
    norm_now = inner(residual, residual)
    for iteration in range(ITERS):
        image_vec = hessian(direction)
        step_size = norm_now / inner(direction, image_vec)
        solution = tuple(sol + step_size * dvec for sol, dvec in zip(solution, direction))
        residual = tuple(res - step_size * ivec for res, ivec in zip(residual, image_vec))
        norm_next = inner(residual, residual)
        direction = tuple(res + (norm_next / norm_now) * dvec for res, dvec in zip(residual, direction))
        norm_now = norm_next
    return (solution[0], solution[1], solution[2])
```

```python
import functools

import jax
import jax.numpy as jnp
from jax import lax
from jax.experimental import pallas as pl
from jax.experimental.pallas import tpu as pltpu
from jax.sharding import PartitionSpec as P

MESH = pl.DeviceIdType.MESH
HI = lax.Precision.HIGHEST
F32 = jnp.float32


def dot(x, y, cx, cy):
    return lax.dot_general(
        x, y, (((cx,), (cy,)), ((), ())), precision=HI, preferred_element_type=F32
    )


def total(x):
    return jnp.sum(jnp.sum(x, axis=0, keepdims=True), axis=1, keepdims=True)


def kernel(
    nrow, ncol,
    tile, coords, counts, damp, fa, fb, fc,
    out_a, out_b, out_c,
    ga, gb, m1, ta1, tb1, m2, ta2, tb2, m3, s2, s3,
    pa, pb, pc, da, db, ra, rb, ia, ib, v0,
    send, recv,
):
    slots, size = tile.shape[0], tile.shape[1]
    rank = fa.shape[0]
    wc = fc.shape[0]
    ka, kb = fa.shape[1] // size, fb.shape[1] // size
    ndev = nrow * ncol
    p, q = lax.axis_index("row"), lax.axis_index("col")
    me = p * ncol + q

    def over_all(k):
        d = lax.rem(me + k, ndev)
        return (lax.div(d, ncol), lax.rem(d, ncol))

    def over_col(k):
        return (p, lax.rem(q + k, ncol))

    def over_row(k):
        return (lax.rem(p + k, nrow), q)

    def spread(src, dst, sem, n, where):
        def one(k, _):
            pltpu.make_async_remote_copy(
                src_ref=src, dst_ref=dst, send_sem=send.at[sem], recv_sem=recv.at[sem],
                device_id=where(k), device_id_type=MESH,
            ).start()
            return 0

        lax.fori_loop(1, n, one, 0)

    def arrived(buf, sem):
        part = buf.at[pl.ds(0, buf.shape[0] - 1)]
        pltpu.make_async_copy(part, part, recv.at[sem]).wait()

    def sent(buf, sem):
        part = buf.at[pl.ds(0, buf.shape[0] - 1)]
        pltpu.make_async_copy(part, part, send.at[sem]).wait()

    barrier = pltpu.get_barrier_semaphore()

    def greet(k, _):
        pl.semaphore_signal(barrier, inc=1, device_id=over_all(k), device_id_type=MESH)
        return 0

    lax.fori_loop(1, ndev, greet, 0)

    row_i = lax.broadcasted_iota(jnp.int32, (rank, 128), 0)
    lane_i = lax.broadcasted_iota(jnp.int32, (rank, 128), 1)
    eye = row_i == lane_i
    msg = m1.shape[1]
    mrow = lax.broadcasted_iota(jnp.int32, (msg, 128), 0)
    mlane = lax.broadcasted_iota(jnp.int32, (msg, 128), 1)

    def as_col(row):
        return jnp.sum(jnp.where(eye, row, 0.0), axis=1, keepdims=True)

    def as_row(col):
        return jnp.sum(jnp.where(eye, col, 0.0), axis=0, keepdims=True)

    first = jnp.where(mlane >= rank, -1.0, jnp.zeros((msg, 128), F32))
    for t in range(slots):
        for c in range(3):
            val = jnp.full((msg, 128), coords[c, t], jnp.int32).astype(F32)
            first = jnp.where((mrow == t) & (mlane == rank + c), val, first)
    m1[me] = first
    m1[me, :wc, :rank] = fc[...]
    for o in range(ka):
        ga[q, o] = fa[:, o * size : (o + 1) * size]
    for o in range(kb):
        gb[p, o] = fb[:, o * size : (o + 1) * size]

    pl.semaphore_wait(barrier, ndev - 1)
    spread(ga.at[q], ga.at[q], 0, ncol, over_col)
    spread(gb.at[p], gb.at[p], 1, nrow, over_row)
    spread(m1.at[me], m1.at[me], 2, ndev, over_all)
    arrived(m1, 2)

    def place(c, dst):
        def one(s, base):
            blk = m1[base + s]
            dst[s] = jnp.broadcast_to(blk[:, rank + c : rank + c + 1], (msg, 128))
            return base

        return one

    lax.fori_loop(0, ncol, place(0, pa), p * ncol)

    def place_b(s, _):
        blk = m1[s * ncol + q]
        pb[s] = jnp.broadcast_to(blk[:, rank + 1 : rank + 2], (msg, 128))
        return 0

    lax.fori_loop(0, nrow, place_b, 0)
    lax.fori_loop(0, ndev, place(2, pc), 0)

    arrived(ga, 0)
    arrived(gb, 1)

    count = counts[0]
    damping = damp[0]

    def splat(val):
        return jnp.full((1, 128), val, jnp.int32).astype(F32)

    my_a = [splat(coords[0, t]) for t in range(slots)]
    my_b = [splat(coords[1, t]) for t in range(slots)]
    my_c = [splat(coords[2, t]) for t in range(slots)]
    own_a = [splat(q * ka + o) for o in range(ka)]
    own_b = [splat(p * kb + o) for o in range(kb)]
    own_c = [splat(me * wc + o) for o in range(wc)]

    def tile_factors(t):
        a, b, k = coords[0, t], coords[1, t], coords[2, t]
        rows_a = ga[lax.div(a, ka), lax.rem(a, ka)]
        rows_b = gb[lax.div(b, kb), lax.rem(b, kb)]
        at = lax.div(k, wc)
        row_c = jnp.sum(jnp.where(mrow + at * wc == k, m1[at], 0.0), axis=0, keepdims=True)
        return rows_a, rows_b, as_col(row_c)

    facs = [tile_factors(t) for t in range(slots)]

    def send_grads(values, ta, tb, m, extra, sem):
        note = extra
        for t in range(slots):
            rows_a, rows_b, col_c = facs[t]
            raw = dot(rows_b, values[t], 1, 1)
            ta[q, t] = raw * col_c
            tb[p, t] = dot(rows_a * col_c, values[t], 1, 0)
            note = jnp.where(
                mrow == t, as_row(jnp.sum(rows_a * raw, axis=1, keepdims=True)), note
            )
        m[me] = note
        spread(ta.at[q], ta.at[q], sem, ncol, over_col)
        spread(tb.at[p], tb.at[p], sem + 1, nrow, over_row)
        spread(m.at[me], m.at[me], sem + 2, ndev, over_all)

    def live(t, x):
        return jnp.where(jnp.full((size, size), t, jnp.int32) < count, x, 0.0)

    values = [
        live(t, tile[t].astype(F32) - dot(facs[t][0], facs[t][1] * facs[t][2], 0, 0))
        for t in range(slots)
    ]
    send_grads(values, ta1, tb1, m2, jnp.zeros((msg, 128), F32), 3)

    def gather_sums(buf, place_ref, n, wanted):
        def one(s, accs):
            accs = list(accs)
            for t in range(slots):
                g = buf[s, t]
                tag = place_ref[s, t : t + 1, :]
                for j, want in enumerate(wanted):
                    accs[j] = accs[j] + g * jnp.where(tag == want, 1.0, 0.0)
            return tuple(accs)

        return lax.fori_loop(
            0, n, one, tuple(jnp.zeros((rank, size), F32) for _ in wanted)
        )

    def depth_sums(m, wanted):
        def one(s, accs):
            g, tag = m[s], pc[s]
            return tuple(acc + jnp.where(tag == w, g, 0.0) for acc, w in zip(accs, wanted))

        accs = lax.fori_loop(
            0, ndev, one, tuple(jnp.zeros((msg, 128), F32) for _ in wanted)
        )
        return [jnp.sum(acc, axis=0, keepdims=True) for acc in accs]

    arrived(ta1, 3)
    for t, x in enumerate(gather_sums(ta1, pa, ncol, my_a)):
        da[t] = x
    for o, x in enumerate(gather_sums(ta1, pa, ncol, own_a)):
        ra[o] = x
    arrived(tb1, 4)
    for t, x in enumerate(gather_sums(tb1, pb, nrow, my_b)):
        db[t] = x
    for o, x in enumerate(gather_sums(tb1, pb, nrow, own_b)):
        rb[o] = x
    arrived(m2, 5)
    depth = depth_sums(m2, my_c + own_c)
    dc, rc = depth[:slots], depth[slots:]

    def inner(xa, xb, xc, ya, yb, yc):
        part = jnp.zeros((rank, size), F32)
        for o in range(ka):
            part += xa(o) * ya(o)
        for o in range(kb):
            part += xb(o) * yb(o)
        res = total(part)
        for o in range(wc):
            res += total(xc[o] * yc[o])
        return res

    get_ra, get_rb = (lambda o: ra[o]), (lambda o: rb[o])
    norm_part = inner(get_ra, get_rb, rc, get_ra, get_rb, rc)

    def product(t, ua, ub, uc):
        rows_a, rows_b, col_c = facs[t]
        left = jnp.concatenate([ua, rows_a], axis=0)
        right = jnp.concatenate([rows_b * col_c, ub * col_c + rows_b * as_col(uc)], axis=0)
        return live(t, dot(left, right, 0, 0))

    curve = jnp.zeros((size, size), F32)
    values = []
    for t in range(slots):
        v = product(t, da[t], db[t], dc[t])
        v0[t] = v
        curve += v * v
        values.append(v)
    extra = jnp.where(
        mrow == slots, norm_part, jnp.where(mrow == slots + 1, total(curve), 0.0)
    )
    send_grads(values, ta2, tb2, m3, extra, 6)

    arrived(ta2, 6)
    for t, x in enumerate(gather_sums(ta2, pa, ncol, my_a)):
        ia[t] = x
    own_ia = gather_sums(ta2, pa, ncol, own_a)
    for o in range(ka):
        ia[slots + o] = own_ia[o]
    arrived(tb2, 7)
    for t, x in enumerate(gather_sums(tb2, pb, nrow, my_b)):
        ib[t] = x
    own_ib = gather_sums(tb2, pb, nrow, own_b)
    for o in range(kb):
        ib[slots + o] = own_ib[o]
    arrived(m3, 8)
    depth = depth_sums(m3, my_c + own_c)
    sums = jnp.sum(m3[...], axis=0)
    norm0 = sums[slots : slots + 1, :]
    curve0 = sums[slots + 1 : slots + 2, :]
    alpha0 = norm0 / (curve0 + damping * norm0)

    def next_residual(res, image):
        return res - alpha0 * (image + damping * res)

    for o in range(ka):
        ia[slots + o] = next_residual(ra[o], ia[slots + o])
    for o in range(kb):
        ib[slots + o] = next_residual(rb[o], ib[slots + o])
    rc1 = [next_residual(rc[o], depth[slots + o]) for o in range(wc)]
    get_a1, get_b1 = (lambda o: ia[slots + o]), (lambda o: ib[slots + o])
    fresh_part = inner(get_a1, get_b1, rc1, get_a1, get_b1, rc1)
    cross_part = inner(get_a1, get_b1, rc1, get_ra, get_rb, rc)
    two = lax.broadcasted_iota(jnp.int32, (2, 128), 0)
    s2[me] = jnp.where(two == 0, fresh_part, cross_part)
    spread(s2.at[me], s2.at[me], 9, ndev, over_all)

    values = [
        product(
            t,
            next_residual(da[t], ia[t]),
            next_residual(db[t], ib[t]),
            next_residual(dc[t], depth[t]),
        )
        for t in range(slots)
    ]
    arrived(s2, 9)
    sums = jnp.sum(s2[...], axis=0)
    fresh, cross = sums[0:1, :], sums[1:2, :]
    beta = fresh / norm0
    curve = jnp.zeros((size, size), F32)
    for t in range(slots):
        v = values[t] + beta * v0[t]
        curve += v * v
    s3[me] = jnp.broadcast_to(total(curve), (1, 128))
    spread(s3.at[me], s3.at[me], 10, ndev, over_all)
    direct = fresh + 2.0 * beta * cross + beta * beta * norm0
    arrived(s3, 10)
    curve1 = jnp.sum(s3[...], axis=0)
    alpha1 = fresh / (curve1 + damping * direct)

    def step(res, res1):
        return alpha0 * res + alpha1 * (res1 + beta * res)

    for o in range(ka):
        out_a[:, o * size : (o + 1) * size] = step(ra[o], ia[slots + o])
    for o in range(kb):
        out_b[:, o * size : (o + 1) * size] = step(rb[o], ib[slots + o])
    for o in range(wc):
        out_c[o : o + 1, :] = step(rc[o], rc1[o])[:, :rank]

    for i, buf in enumerate((ga, gb, m1, ta1, tb1, m2, ta2, tb2, m3, s2, s3)):
        sent(buf, i)


def per_device(
    nrow, ncol, tile_data, tile_coords, tile_counts, factor_rows, factor_cols, factor_depth, damping
):
    slots, size, _ = tile_data.shape
    rank, wa = factor_rows.shape
    wb, wc = factor_cols.shape[1], factor_depth.shape[1]
    ka, kb = wa // size, wb // size
    ndev = nrow * ncol
    msg = -(-max(wc, slots + 2) // 8) * 8
    vm = pltpu.VMEM
    exchange = [
        vm((ncol, slots, rank, size), F32),
        vm((nrow, slots, rank, size), F32),
        vm((ndev, msg, 128), F32),
    ]
    vspec = pl.BlockSpec(memory_space=pltpu.VMEM)
    sspec = pl.BlockSpec(memory_space=pltpu.SMEM)
    step_a, step_b, step_c = pl.pallas_call(
        functools.partial(kernel, nrow, ncol),
        out_shape=(
            jax.ShapeDtypeStruct((rank, wa), F32),
            jax.ShapeDtypeStruct((rank, wb), F32),
            jax.ShapeDtypeStruct((wc, rank), F32),
        ),
        in_specs=[vspec, sspec, sspec, sspec, vspec, vspec, vspec],
        out_specs=(vspec, vspec, vspec),
        scratch_shapes=[
            vm((ncol, ka, rank, size), F32),
            vm((nrow, kb, rank, size), F32),
            vm((ndev, msg, 128), F32),
            *exchange,
            *exchange,
            vm((ndev, 2, 128), F32),
            vm((ndev, 1, 128), F32),
            vm((ncol, msg, 128), F32),
            vm((nrow, msg, 128), F32),
            vm((ndev, msg, 128), F32),
            vm((slots, rank, size), F32),
            vm((slots, rank, size), F32),
            vm((ka, rank, size), F32),
            vm((kb, rank, size), F32),
            vm((slots + ka, rank, size), F32),
            vm((slots + kb, rank, size), F32),
            vm((slots, size, size), F32),
            pltpu.SemaphoreType.DMA((11,)),
            pltpu.SemaphoreType.DMA((11,)),
        ],
        compiler_params=pltpu.CompilerParams(collective_id=0, has_side_effects=True),
    )(
        tile_data, tile_coords, tile_counts, damping.reshape(1),
        factor_rows, factor_cols, factor_depth.T,
    )
    return step_a, step_b, step_c.T


def solution(mesh):
    nrow, ncol = mesh.shape["row"], mesh.shape["col"]
    return jax.shard_map(
        functools.partial(per_device, nrow, ncol),
        mesh=mesh,
        in_specs=(
            P(("row", "col"), None, None),
            P(None, ("row", "col")),
            P(("row", "col")),
            P(None, ("row", "col")),
            P(None, ("col", "row")),
            P(None, ("row", "col")),
            P(),
        ),
        out_specs=(P(None, ("row", "col")), P(None, ("col", "row")), P(None, ("row", "col"))),
        check_vma=False,
    )
```

```python
import functools

import jax
import jax.numpy as jnp
from jax import lax
from jax.experimental import pallas as pl
from jax.experimental.pallas import tpu as pltpu
from jax.sharding import PartitionSpec as P

MESH = pl.DeviceIdType.MESH
CORES = 2
HI = lax.Precision.HIGHEST
F32 = jnp.float32


def dot(x, y, cx, cy):
    return lax.dot_general(
        x, y, (((cx,), (cy,)), ((), ())), precision=HI, preferred_element_type=F32
    )


def total(x):
    return jnp.sum(jnp.sum(x, axis=0, keepdims=True), axis=1, keepdims=True)


def kernel(
    nrow, ncol,
    tile, coords, counts, damp, fa, fb, fc,
    out_a, out_b, out_c,
    ga, gb, m1, ta1, tb1, m2, ta2, tb2, m3, s2, s3,
    pa, pb, pc, da, db, ra, rb, ia, ib, v0,
    send, recv, ls0, lr0, ls1, lr1, ls2, lr2,
):
    slots, size = tile.shape[0], tile.shape[1]
    rank = fa.shape[0]
    wc = fc.shape[0]
    ka, kb = fa.shape[1] // size, fb.shape[1] // size
    ndev = nrow * ncol
    p, q = lax.axis_index("row"), lax.axis_index("col")
    me = p * ncol + q

    def over_all(k):
        d = lax.rem(me + k, ndev)
        return (lax.div(d, ncol), lax.rem(d, ncol))

    def over_col(k):
        return (p, lax.rem(q + k, ncol))

    def over_row(k):
        return (lax.rem(p + k, nrow), q)

    def spread(src, dst, sem, n, where):
        def one(k, _):
            pltpu.make_async_remote_copy(
                src_ref=src, dst_ref=dst, send_sem=send.at[sem], recv_sem=recv.at[sem],
                device_id=where(k), device_id_type=MESH,
            ).start()
            return 0

        lax.fori_loop(1, n, one, 0)

    def arrived(buf, sem):
        part = buf.at[pl.ds(0, buf.shape[0] - 1)]
        pltpu.make_async_copy(part, part, recv.at[sem]).wait()

    def sent(buf, sem):
        part = buf.at[pl.ds(0, buf.shape[0] - 1)]
        pltpu.make_async_copy(part, part, send.at[sem]).wait()

    nz = ncol // CORES
    z, core = lax.div(q, CORES), lax.rem(q, CORES)
    other = CORES - 1 - core

    def move(buf, ls, lr, dz, block, chunk):
        target = (q + CORES, q - CORES, z * CORES + other)[dz]
        piece = buf.at[block * CORES + core, chunk]
        return pltpu.make_async_remote_copy(
            src_ref=piece, dst_ref=piece,
            send_sem=ls.at[dz, block, chunk], recv_sem=lr.at[block * CORES + core, chunk],
            device_id=(p, target), device_id_type=MESH,
        )

    def line_start(buf, ls, lr):
        for chunk in range(buf.shape[1]):
            @pl.when(z + 1 < nz)
            def _():
                move(buf, ls, lr, 0, z, chunk).start()

            @pl.when(z > 0)
            def _():
                move(buf, ls, lr, 1, z, chunk).start()

            move(buf, ls, lr, 2, z, chunk).start()

    def line_relay(buf, ls, lr):
        chunks = buf.shape[1]

        def landed(slot, chunk):
            piece = buf.at[slot, chunk]
            pltpu.make_async_copy(piece, piece, lr.at[slot, chunk]).wait()

        def one(d, _):
            for chunk in range(chunks):
                @pl.when(z - d >= 0)
                def _():
                    block = z - d
                    landed(block * CORES + core, chunk)

                    @pl.when(z + 1 < nz)
                    def _():
                        move(buf, ls, lr, 0, block, chunk).start()

                    move(buf, ls, lr, 2, block, chunk).start()

                @pl.when(z + d < nz)
                def _():
                    block = z + d
                    landed(block * CORES + core, chunk)

                    @pl.when(z > 0)
                    def _():
                        move(buf, ls, lr, 1, block, chunk).start()

                    move(buf, ls, lr, 2, block, chunk).start()

            return 0

        lax.fori_loop(1, nz, one, 0)

        def rest(block, _):
            for chunk in range(chunks):
                landed(block * CORES + other, chunk)
            return 0

        lax.fori_loop(0, nz, rest, 0)

    def line_sent(buf, ls, lr):
        def one(block, _):
            for chunk in range(buf.shape[1]):
                @pl.when((z + 1 < nz) & (block <= z))
                def _():
                    move(buf, ls, lr, 0, block, chunk).wait_send()

                @pl.when((z > 0) & (block >= z))
                def _():
                    move(buf, ls, lr, 1, block, chunk).wait_send()

                move(buf, ls, lr, 2, block, chunk).wait_send()
            return 0

        lax.fori_loop(0, nz, one, 0)

    barrier = pltpu.get_barrier_semaphore()

    def greet(k, _):
        pl.semaphore_signal(barrier, inc=1, device_id=over_all(k), device_id_type=MESH)
        return 0

    lax.fori_loop(1, ndev, greet, 0)

    row_i = lax.broadcasted_iota(jnp.int32, (rank, 128), 0)
    lane_i = lax.broadcasted_iota(jnp.int32, (rank, 128), 1)
    eye = row_i == lane_i
    msg = m1.shape[1]
    mrow = lax.broadcasted_iota(jnp.int32, (msg, 128), 0)
    mlane = lax.broadcasted_iota(jnp.int32, (msg, 128), 1)
    nrow_i = lax.broadcasted_iota(jnp.int32, (slots, 128), 0)
    nlane = lax.broadcasted_iota(jnp.int32, (slots, 128), 1)

    def as_col(row):
        return jnp.sum(jnp.where(eye, row, 0.0), axis=1, keepdims=True)

    def as_row(col):
        return jnp.sum(jnp.where(eye, col, 0.0), axis=0, keepdims=True)

    first = jnp.where(mlane >= rank, -1.0, jnp.zeros((msg, 128), F32))
    for t in range(slots):
        for c in range(3):
            val = jnp.full((msg, 128), coords[c, t], jnp.int32).astype(F32)
            first = jnp.where((mrow == t) & (mlane == rank + c), val, first)
    m1[me] = first
    m1[me, :wc, :rank] = fc[...]
    for o in range(ka):
        ga[q, o] = fa[:, o * size : (o + 1) * size]
    for o in range(kb):
        gb[p, o] = fb[:, o * size : (o + 1) * size]

    pl.semaphore_wait(barrier, ndev - 1)
    spread(m1.at[me], m1.at[me], 2, ndev, over_all)
    line_start(ga, ls0, lr0)
    spread(gb.at[p], gb.at[p], 1, nrow, over_row)
    line_relay(ga, ls0, lr0)
    arrived(m1, 2)

    def place(c, dst):
        def one(s, base):
            blk = m1[base + s]
            dst[s] = jnp.broadcast_to(blk[:, rank + c : rank + c + 1], (msg, 128))
            return base

        return one

    lax.fori_loop(0, ncol, place(0, pa), p * ncol)

    def place_b(s, _):
        blk = m1[s * ncol + q]
        pb[s] = jnp.broadcast_to(blk[:, rank + 1 : rank + 2], (msg, 128))
        return 0

    lax.fori_loop(0, nrow, place_b, 0)
    lax.fori_loop(0, ndev, place(2, pc), 0)

    arrived(gb, 1)

    count = counts[0]
    damping = damp[0]

    def splat(val):
        return jnp.full((1, 128), val, jnp.int32).astype(F32)

    my_a = [splat(coords[0, t]) for t in range(slots)]
    my_b = [splat(coords[1, t]) for t in range(slots)]
    my_c = [splat(coords[2, t]) for t in range(slots)]
    own_a = [splat(q * ka + o) for o in range(ka)]
    own_b = [splat(p * kb + o) for o in range(kb)]
    own_c = [splat(me * wc + o) for o in range(wc)]

    def tile_factors(t):
        a, b, k = coords[0, t], coords[1, t], coords[2, t]
        rows_a = ga[lax.div(a, ka), lax.rem(a, ka)]
        rows_b = gb[lax.div(b, kb), lax.rem(b, kb)]
        at = lax.div(k, wc)
        row_c = jnp.sum(jnp.where(mrow + at * wc == k, m1[at], 0.0), axis=0, keepdims=True)
        return rows_a, rows_b, as_col(row_c)

    facs = [tile_factors(t) for t in range(slots)]

    def send_grads(values, ta, tb, m, extra, sem, ls, lr):
        note = extra
        for t in range(slots):
            rows_a, rows_b, col_c = facs[t]
            raw = dot(rows_b, values[t], 1, 1)
            ta[q, t] = raw * col_c
            tb[p, t] = dot(rows_a * col_c, values[t], 1, 0)
            note = jnp.where(
                (nrow_i == t) & (nlane < rank),
                as_row(jnp.sum(rows_a * raw, axis=1, keepdims=True)), note,
            )
        m[me] = note
        spread(m.at[me], m.at[me], sem + 2, ndev, over_all)
        line_start(ta, ls, lr)
        spread(tb.at[p], tb.at[p], sem + 1, nrow, over_row)

    def live(t, x):
        return jnp.where(jnp.full((size, size), t, jnp.int32) < count, x, 0.0)

    values = [
        live(t, tile[t].astype(F32) - dot(facs[t][0], facs[t][1] * facs[t][2], 0, 0))
        for t in range(slots)
    ]
    send_grads(values, ta1, tb1, m2, jnp.zeros((slots, 128), F32), 3, ls1, lr1)

    def gather_sums(buf, place_ref, n, wanted):
        def one(s, accs):
            accs = list(accs)
            for t in range(slots):
                g = buf[s, t]
                tag = place_ref[s, t : t + 1, :]
                for j, want in enumerate(wanted):
                    accs[j] = accs[j] + g * jnp.where(tag == want, 1.0, 0.0)
            return tuple(accs)

        return lax.fori_loop(
            0, n, one, tuple(jnp.zeros((rank, size), F32) for _ in wanted)
        )

    def depth_sums(m, wanted):
        def one(s, accs):
            g, tag = m[s], pc[s, :slots]
            return tuple(acc + jnp.where(tag == w, g, 0.0) for acc, w in zip(accs, wanted))

        accs = lax.fori_loop(
            0, ndev, one, tuple(jnp.zeros((slots, 128), F32) for _ in wanted)
        )
        return [
            jnp.sum(jnp.where(nlane < rank, acc, 0.0), axis=0, keepdims=True) for acc in accs
        ]

    line_relay(ta1, ls1, lr1)
    for t, x in enumerate(gather_sums(ta1, pa, ncol, my_a)):
        da[t] = x
    for o, x in enumerate(gather_sums(ta1, pa, ncol, own_a)):
        ra[o] = x
    arrived(tb1, 4)
    for t, x in enumerate(gather_sums(tb1, pb, nrow, my_b)):
        db[t] = x
    for o, x in enumerate(gather_sums(tb1, pb, nrow, own_b)):
        rb[o] = x
    arrived(m2, 5)
    depth = depth_sums(m2, my_c + own_c)
    dc, rc = depth[:slots], depth[slots:]

    def inner(xa, xb, xc, ya, yb, yc):
        part = jnp.zeros((rank, size), F32)
        for o in range(ka):
            part += xa(o) * ya(o)
        for o in range(kb):
            part += xb(o) * yb(o)
        res = total(part)
        for o in range(wc):
            res += total(xc[o] * yc[o])
        return res

    get_ra, get_rb = (lambda o: ra[o]), (lambda o: rb[o])
    norm_part = inner(get_ra, get_rb, rc, get_ra, get_rb, rc)

    def product(t, ua, ub, uc):
        rows_a, rows_b, col_c = facs[t]
        left = jnp.concatenate([ua, rows_a], axis=0)
        right = jnp.concatenate([rows_b * col_c, ub * col_c + rows_b * as_col(uc)], axis=0)
        return live(t, dot(left, right, 0, 0))

    curve = jnp.zeros((size, size), F32)
    values = []
    for t in range(slots):
        v = product(t, da[t], db[t], dc[t])
        v0[t] = v
        curve += v * v
        values.append(v)
    extra = jnp.where(
        nlane == rank, norm_part, jnp.where(nlane == rank + 1, total(curve), 0.0)
    )
    send_grads(values, ta2, tb2, m3, extra, 6, ls2, lr2)

    line_relay(ta2, ls2, lr2)
    for t, x in enumerate(gather_sums(ta2, pa, ncol, my_a)):
        ia[t] = x
    own_ia = gather_sums(ta2, pa, ncol, own_a)
    for o in range(ka):
        ia[slots + o] = own_ia[o]
    arrived(tb2, 7)
    for t, x in enumerate(gather_sums(tb2, pb, nrow, my_b)):
        ib[t] = x
    own_ib = gather_sums(tb2, pb, nrow, own_b)
    for o in range(kb):
        ib[slots + o] = own_ib[o]
    arrived(m3, 8)
    depth = depth_sums(m3, my_c + own_c)
    sums = jnp.sum(m3[...], axis=0)
    norm0 = jnp.broadcast_to(sums[0:1, rank : rank + 1], (1, 128))
    curve0 = jnp.broadcast_to(sums[0:1, rank + 1 : rank + 2], (1, 128))
    alpha0 = norm0 / (curve0 + damping * norm0)

    def next_residual(res, image):
        return res - alpha0 * (image + damping * res)

    for o in range(ka):
        ia[slots + o] = next_residual(ra[o], ia[slots + o])
    for o in range(kb):
        ib[slots + o] = next_residual(rb[o], ib[slots + o])
    rc1 = [next_residual(rc[o], depth[slots + o]) for o in range(wc)]
    get_a1, get_b1 = (lambda o: ia[slots + o]), (lambda o: ib[slots + o])
    fresh_part = inner(get_a1, get_b1, rc1, get_a1, get_b1, rc1)
    cross_part = inner(get_a1, get_b1, rc1, get_ra, get_rb, rc)
    two = lax.broadcasted_iota(jnp.int32, (2, 128), 0)
    s2[me] = jnp.where(two == 0, fresh_part, cross_part)
    spread(s2.at[me], s2.at[me], 9, ndev, over_all)

    values = [
        product(
            t,
            next_residual(da[t], ia[t]),
            next_residual(db[t], ib[t]),
            next_residual(dc[t], depth[t]),
        )
        for t in range(slots)
    ]
    arrived(s2, 9)
    sums = jnp.sum(s2[...], axis=0)
    fresh, cross = sums[0:1, :], sums[1:2, :]
    beta = fresh / norm0
    curve = jnp.zeros((size, size), F32)
    for t in range(slots):
        v = values[t] + beta * v0[t]
        curve += v * v
    s3[me] = jnp.broadcast_to(total(curve), (1, 128))
    spread(s3.at[me], s3.at[me], 10, ndev, over_all)
    direct = fresh + 2.0 * beta * cross + beta * beta * norm0
    arrived(s3, 10)
    curve1 = jnp.sum(s3[...], axis=0)
    alpha1 = fresh / (curve1 + damping * direct)

    def step(res, res1):
        return alpha0 * res + alpha1 * (res1 + beta * res)

    for o in range(ka):
        out_a[:, o * size : (o + 1) * size] = step(ra[o], ia[slots + o])
    for o in range(kb):
        out_b[:, o * size : (o + 1) * size] = step(rb[o], ib[slots + o])
    for o in range(wc):
        out_c[o : o + 1, :] = step(rc[o], rc1[o])[:, :rank]

    line_sent(ga, ls0, lr0)
    line_sent(ta1, ls1, lr1)
    line_sent(ta2, ls2, lr2)
    for i, buf in ((1, gb), (2, m1), (4, tb1), (5, m2), (7, tb2), (8, m3), (9, s2), (10, s3)):
        sent(buf, i)


def per_device(
    nrow, ncol, tile_data, tile_coords, tile_counts, factor_rows, factor_cols, factor_depth, damping
):
    slots, size, _ = tile_data.shape
    rank, wa = factor_rows.shape
    wb, wc = factor_cols.shape[1], factor_depth.shape[1]
    ka, kb = wa // size, wb // size
    ndev = nrow * ncol
    msg = -(-max(wc, slots) // 8) * 8
    vm = pltpu.VMEM
    exchange = [
        vm((ncol, slots, rank, size), F32),
        vm((nrow, slots, rank, size), F32),
        vm((ndev, slots, 128), F32),
    ]

    def line(chunks):
        return [
            pltpu.SemaphoreType.DMA((3, ncol // CORES, chunks)),
            pltpu.SemaphoreType.DMA((ncol, chunks)),
        ]

    vspec = pl.BlockSpec(memory_space=pltpu.VMEM)
    sspec = pl.BlockSpec(memory_space=pltpu.SMEM)
    step_a, step_b, step_c = pl.pallas_call(
        functools.partial(kernel, nrow, ncol),
        out_shape=(
            jax.ShapeDtypeStruct((rank, wa), F32),
            jax.ShapeDtypeStruct((rank, wb), F32),
            jax.ShapeDtypeStruct((wc, rank), F32),
        ),
        in_specs=[vspec, sspec, sspec, sspec, vspec, vspec, vspec],
        out_specs=(vspec, vspec, vspec),
        scratch_shapes=[
            vm((ncol, ka, rank, size), F32),
            vm((nrow, kb, rank, size), F32),
            vm((ndev, msg, 128), F32),
            *exchange,
            *exchange,
            vm((ndev, 2, 128), F32),
            vm((ndev, 1, 128), F32),
            vm((ncol, msg, 128), F32),
            vm((nrow, msg, 128), F32),
            vm((ndev, msg, 128), F32),
            vm((slots, rank, size), F32),
            vm((slots, rank, size), F32),
            vm((ka, rank, size), F32),
            vm((kb, rank, size), F32),
            vm((slots + ka, rank, size), F32),
            vm((slots + kb, rank, size), F32),
            vm((slots, size, size), F32),
            pltpu.SemaphoreType.DMA((11,)),
            pltpu.SemaphoreType.DMA((11,)),
            *line(ka),
            *line(slots),
            *line(slots),
        ],
        compiler_params=pltpu.CompilerParams(collective_id=0, has_side_effects=True),
    )(
        tile_data, tile_coords, tile_counts, damping.reshape(1),
        factor_rows, factor_cols, factor_depth.T,
    )
    return step_a, step_b, step_c.T


def solution(mesh):
    nrow, ncol = mesh.shape["row"], mesh.shape["col"]
    return jax.shard_map(
        functools.partial(per_device, nrow, ncol),
        mesh=mesh,
        in_specs=(
            P(("row", "col"), None, None),
            P(None, ("row", "col")),
            P(("row", "col")),
            P(None, ("row", "col")),
            P(None, ("col", "row")),
            P(None, ("row", "col")),
            P(),
        ),
        out_specs=(P(None, ("row", "col")), P(None, ("col", "row")), P(None, ("row", "col"))),
        check_vma=False,
    )
```

```python
import functools

import jax
import jax.numpy as jnp
from jax import lax
from jax.experimental import pallas as pl
from jax.experimental.pallas import tpu as pltpu
from jax.sharding import PartitionSpec as P

MESH = pl.DeviceIdType.MESH
CORES = 2
HI = lax.Precision.HIGHEST
F32 = jnp.float32


def dot(x, y, cx, cy):
    return lax.dot_general(
        x, y, (((cx,), (cy,)), ((), ())), precision=HI, preferred_element_type=F32
    )


def total(x):
    return jnp.sum(jnp.sum(x, axis=0, keepdims=True), axis=1, keepdims=True)


def kernel(
    nrow, ncol,
    tile, coords, counts, damp, fa, fb, fc,
    out_a, out_b, out_c,
    ga, gb, m1, ta1, tb1, m2, ta2, tb2, m3, s2,
    pa, pb, pc, da, db, ia, ib, v0,
    send, recv, ls0, lr0, ls1, lr1, ls2, lr2,
):
    slots, size = tile.shape[0], tile.shape[1]
    rank = fa.shape[0]
    wc = fc.shape[0]
    ka, kb = fa.shape[1] // size, fb.shape[1] // size
    ndev = nrow * ncol
    p, q = lax.axis_index("row"), lax.axis_index("col")
    me = p * ncol + q

    def over_all(k):
        d = lax.rem(me + k, ndev)
        return (lax.div(d, ncol), lax.rem(d, ncol))

    def over_col(k):
        return (p, lax.rem(q + k, ncol))

    def over_row(k):
        return (lax.rem(p + k, nrow), q)

    def spread(src, dst, sem, n, where):
        def one(k, _):
            pltpu.make_async_remote_copy(
                src_ref=src, dst_ref=dst, send_sem=send.at[sem], recv_sem=recv.at[sem],
                device_id=where(k), device_id_type=MESH,
            ).start()
            return 0

        lax.fori_loop(1, n, one, 0)

    def arrived(buf, sem):
        part = buf.at[pl.ds(0, buf.shape[0] - 1)]
        pltpu.make_async_copy(part, part, recv.at[sem]).wait()

    def sent(buf, sem):
        part = buf.at[pl.ds(0, buf.shape[0] - 1)]
        pltpu.make_async_copy(part, part, send.at[sem]).wait()

    nz = ncol // CORES
    z, core = lax.div(q, CORES), lax.rem(q, CORES)
    other = CORES - 1 - core

    def move(buf, ls, lr, dz, block, chunk):
        target = (q + CORES, q - CORES, z * CORES + other)[dz]
        piece = buf.at[block * CORES + core, chunk]
        return pltpu.make_async_remote_copy(
            src_ref=piece, dst_ref=piece,
            send_sem=ls.at[dz, block, chunk], recv_sem=lr.at[block * CORES + core, chunk],
            device_id=(p, target), device_id_type=MESH,
        )

    def line_start(buf, ls, lr, chunks):
        for chunk in chunks:
            @pl.when(z + 1 < nz)
            def _():
                move(buf, ls, lr, 0, z, chunk).start()

            @pl.when(z > 0)
            def _():
                move(buf, ls, lr, 1, z, chunk).start()

            move(buf, ls, lr, 2, z, chunk).start()

    def line_relay(buf, ls, lr, use, between):
        chunks = range(buf.shape[1])

        def landed(slot, chunk):
            piece = buf.at[slot, chunk]
            pltpu.make_async_copy(piece, piece, lr.at[slot, chunk]).wait()

        def relay(d):
            for chunk in chunks:
                @pl.when(z - d >= 0)
                def _():
                    block = z - d
                    landed(block * CORES + core, chunk)

                    @pl.when(z + 1 < nz)
                    def _():
                        move(buf, ls, lr, 0, block, chunk).start()

                    move(buf, ls, lr, 2, block, chunk).start()

                @pl.when(z + d < nz)
                def _():
                    block = z + d
                    landed(block * CORES + core, chunk)

                    @pl.when(z > 0)
                    def _():
                        move(buf, ls, lr, 1, block, chunk).start()

                    move(buf, ls, lr, 2, block, chunk).start()

                @pl.when(z - d >= 0)
                def _():
                    use((z - d) * CORES + core, chunk)

                @pl.when(z + d < nz)
                def _():
                    use((z + d) * CORES + core, chunk)

        def partner(d):
            for chunk in chunks:
                @pl.when(z - d >= 0)
                def _():
                    landed((z - d) * CORES + other, chunk)
                    use((z - d) * CORES + other, chunk)

                @pl.when((z + d < nz) & (d > 0))
                def _():
                    landed((z + d) * CORES + other, chunk)
                    use((z + d) * CORES + other, chunk)

        def stage(d, _):
            relay(d)
            partner(d - 1)
            return 0

        for chunk in chunks:
            use(q, chunk)
        lax.fori_loop(1, nz - 1, stage, 0)
        between()
        lax.fori_loop(nz - 1, nz, stage, 0)
        partner(nz - 1)

    def line_sent(buf, ls, lr):
        def one(block, _):
            for chunk in range(buf.shape[1]):
                @pl.when((z + 1 < nz) & (block <= z))
                def _():
                    move(buf, ls, lr, 0, block, chunk).wait_send()

                @pl.when((z > 0) & (block >= z))
                def _():
                    move(buf, ls, lr, 1, block, chunk).wait_send()

                move(buf, ls, lr, 2, block, chunk).wait_send()
            return 0

        lax.fori_loop(0, nz, one, 0)

    barrier = pltpu.get_barrier_semaphore()

    def greet(k, _):
        pl.semaphore_signal(barrier, inc=1, device_id=over_all(k), device_id_type=MESH)
        return 0

    lax.fori_loop(1, ndev, greet, 0)

    row_i = lax.broadcasted_iota(jnp.int32, (rank, 128), 0)
    lane_i = lax.broadcasted_iota(jnp.int32, (rank, 128), 1)
    eye = row_i == lane_i
    msg = m1.shape[1]
    mrow = lax.broadcasted_iota(jnp.int32, (msg, 128), 0)
    mlane = lax.broadcasted_iota(jnp.int32, (msg, 128), 1)
    nrow_i = lax.broadcasted_iota(jnp.int32, (slots, 128), 0)
    nlane = lax.broadcasted_iota(jnp.int32, (slots, 128), 1)

    def as_col(row):
        return jnp.sum(jnp.where(eye, row, 0.0), axis=1, keepdims=True)

    def as_row(col):
        return jnp.sum(jnp.where(eye, col, 0.0), axis=0, keepdims=True)

    first = jnp.where(mlane >= rank, -1.0, jnp.zeros((msg, 128), F32))
    for t in range(slots):
        for c in range(3):
            val = jnp.full((msg, 128), coords[c, t], jnp.int32).astype(F32)
            first = jnp.where((mrow == t) & (mlane == rank + c), val, first)
    m1[me] = first
    m1[me, :wc, :rank] = fc[...]
    for o in range(ka):
        ga[q, o] = fa[:, o * size : (o + 1) * size]
    for o in range(kb):
        gb[p, o] = fb[:, o * size : (o + 1) * size]

    pl.semaphore_wait(barrier, ndev - 1)
    spread(m1.at[me], m1.at[me], 2, ndev, over_all)
    line_start(ga, ls0, lr0, range(ka))
    spread(gb.at[p], gb.at[p], 1, nrow, over_row)

    def place(c, dst):
        def one(s, base):
            blk = m1[base + s]
            dst[s] = jnp.broadcast_to(blk[:, rank + c : rank + c + 1], (msg, 128))
            return base

        return one


    def place_b(s, _):
        blk = m1[s * ncol + q]
        pb[s] = jnp.broadcast_to(blk[:, rank + 1 : rank + 2], (msg, 128))
        return 0

    def place_all():
        arrived(m1, 2)
        lax.fori_loop(0, ncol, place(0, pa), p * ncol)
        lax.fori_loop(0, nrow, place_b, 0)
        lax.fori_loop(0, ndev, place(2, pc), 0)
        arrived(gb, 1)

    line_relay(ga, ls0, lr0, lambda slot, chunk: None, place_all)

    count = counts[0]
    damping = damp[0]

    def splat(val):
        return jnp.full((1, 128), val, jnp.int32).astype(F32)

    my_a = [splat(coords[0, t]) for t in range(slots)]
    my_b = [splat(coords[1, t]) for t in range(slots)]
    my_c = [splat(coords[2, t]) for t in range(slots)]
    own_a = [splat(q * ka + o) for o in range(ka)]
    own_b = [splat(p * kb + o) for o in range(kb)]
    own_c = [splat(me * wc + o) for o in range(wc)]

    def tile_factors(t):
        a, b, k = coords[0, t], coords[1, t], coords[2, t]
        rows_a = ga[lax.div(a, ka), lax.rem(a, ka)]
        rows_b = gb[lax.div(b, kb), lax.rem(b, kb)]
        at = lax.div(k, wc)
        row_c = jnp.sum(jnp.where(mrow + at * wc == k, m1[at], 0.0), axis=0, keepdims=True)
        return rows_a, rows_b, as_col(row_c)

    facs = [tile_factors(t) for t in range(slots)]

    def send_grads(values, ta, tb, m, extra, sem, ls, lr):
        note = extra
        for t in range(slots):
            rows_a, rows_b, col_c = facs[t]
            raw = dot(rows_b, values[t], 1, 1)
            ta[q, t] = raw * col_c
            line_start(ta, ls, lr, (t,))
            tb[p, t] = dot(rows_a * col_c, values[t], 1, 0)
            note = jnp.where(
                (nrow_i == t) & (nlane < rank),
                as_row(jnp.sum(rows_a * raw, axis=1, keepdims=True)), note,
            )
        m[me] = note
        spread(m.at[me], m.at[me], sem + 2, ndev, over_all)
        spread(tb.at[p], tb.at[p], sem + 1, nrow, over_row)

    def live(t, x):
        return jnp.where(jnp.full((size, size), t, jnp.int32) < count, x, 0.0)

    values = [
        live(t, tile[t].astype(F32) - dot(facs[t][0], facs[t][1] * facs[t][2], 0, 0))
        for t in range(slots)
    ]
    send_grads(values, ta1, tb1, m2, jnp.zeros((slots, 128), F32), 3, ls1, lr1)

    def take(acc, buf, tags, wanted):
        def one(slot, chunk):
            g = buf[slot, chunk]
            tag = tags[slot, chunk : chunk + 1, :]
            for i, want in enumerate(wanted):
                acc[i] += g * jnp.where(tag == want, 1.0, 0.0)

        return one

    def collect(ta, tb, m, ls, lr, sem, acc_a, acc_b):
        acc_a[...] = jnp.zeros_like(acc_a)
        acc_b[...] = jnp.zeros_like(acc_b)
        take_b = take(acc_b, tb, pb, my_b + own_b)
        depth = []

        def row_sums(s, _):
            for t in range(slots):
                take_b(s, t)
            return 0

        def between():
            arrived(m, sem + 2)
            depth.extend(depth_sums(m, my_c + own_c))
            arrived(tb, sem + 1)
            lax.fori_loop(0, nrow, row_sums, 0)

        line_relay(ta, ls, lr, take(acc_a, ta, pa, my_a + own_a), between)
        return depth

    def depth_sums(m, wanted):
        def one(s, accs):
            g, tag = m[s], pc[s, :slots]
            return tuple(acc + jnp.where(tag == w, g, 0.0) for acc, w in zip(accs, wanted))

        accs = lax.fori_loop(
            0, ndev, one, tuple(jnp.zeros((slots, 128), F32) for _ in wanted)
        )
        return [
            jnp.sum(jnp.where(nlane < rank, acc, 0.0), axis=0, keepdims=True) for acc in accs
        ]

    depth = collect(ta1, tb1, m2, ls1, lr1, 3, da, db)
    dc, rc = depth[:slots], depth[slots:]

    def inner(xa, xb, xc, ya, yb, yc):
        part = jnp.zeros((rank, size), F32)
        for o in range(ka):
            part += xa(o) * ya(o)
        for o in range(kb):
            part += xb(o) * yb(o)
        res = total(part)
        for o in range(wc):
            res += total(xc[o] * yc[o])
        return res

    get_ra, get_rb = (lambda o: da[slots + o]), (lambda o: db[slots + o])
    norm_part = inner(get_ra, get_rb, rc, get_ra, get_rb, rc)

    def product(t, ua, ub, uc):
        rows_a, rows_b, col_c = facs[t]
        left = jnp.concatenate([ua, rows_a], axis=0)
        right = jnp.concatenate([rows_b * col_c, ub * col_c + rows_b * as_col(uc)], axis=0)
        return live(t, dot(left, right, 0, 0))

    curve = jnp.zeros((size, size), F32)
    values = []
    for t in range(slots):
        v = product(t, da[t], db[t], dc[t])
        v0[t] = v
        curve += v * v
        values.append(v)
    extra = jnp.where(
        nlane == rank, norm_part, jnp.where(nlane == rank + 1, total(curve), 0.0)
    )
    send_grads(values, ta2, tb2, m3, extra, 6, ls2, lr2)

    depth = collect(ta2, tb2, m3, ls2, lr2, 6, ia, ib)
    sums = jnp.sum(m3[...], axis=0)
    norm0 = jnp.broadcast_to(sums[0:1, rank : rank + 1], (1, 128))
    curve0 = jnp.broadcast_to(sums[0:1, rank + 1 : rank + 2], (1, 128))
    alpha0 = norm0 / (curve0 + damping * norm0)

    def next_residual(res, image):
        return res - alpha0 * (image + damping * res)

    for o in range(ka):
        ia[slots + o] = next_residual(da[slots + o], ia[slots + o])
    for o in range(kb):
        ib[slots + o] = next_residual(db[slots + o], ib[slots + o])
    rc1 = [next_residual(rc[o], depth[slots + o]) for o in range(wc)]
    get_a1, get_b1 = (lambda o: ia[slots + o]), (lambda o: ib[slots + o])
    fresh_part = inner(get_a1, get_b1, rc1, get_a1, get_b1, rc1)
    cross_part = inner(get_a1, get_b1, rc1, get_ra, get_rb, rc)
    curve_part = jnp.zeros((size, size), F32)
    mixed_part = jnp.zeros((size, size), F32)
    for t in range(slots):
        v = product(
            t,
            next_residual(da[t], ia[t]),
            next_residual(db[t], ib[t]),
            next_residual(dc[t], depth[t]),
        )
        curve_part += v * v
        mixed_part += v * v0[t]
    parts = (fresh_part, cross_part, total(curve_part), total(mixed_part))
    for i, part in enumerate(parts):
        s2[me, i : i + 1, :] = jnp.broadcast_to(part, (1, 128))
    spread(s2.at[me], s2.at[me], 9, ndev, over_all)
    arrived(s2, 9)
    sums = jnp.sum(s2[...], axis=0)
    fresh, cross, curve_r, mixed = (sums[i : i + 1, :] for i in range(4))
    beta = fresh / norm0
    direct = fresh + beta * (2.0 * cross + beta * norm0)
    curve1 = curve_r + beta * (2.0 * mixed + beta * curve0)
    alpha1 = fresh / (curve1 + damping * direct)

    def step(res, res1):
        return alpha0 * res + alpha1 * (res1 + beta * res)

    for o in range(ka):
        out_a[:, o * size : (o + 1) * size] = step(da[slots + o], ia[slots + o])
    for o in range(kb):
        out_b[:, o * size : (o + 1) * size] = step(db[slots + o], ib[slots + o])
    for o in range(wc):
        out_c[o : o + 1, :] = step(rc[o], rc1[o])[:, :rank]

    line_sent(ga, ls0, lr0)
    line_sent(ta1, ls1, lr1)
    line_sent(ta2, ls2, lr2)
    for i, buf in ((1, gb), (2, m1), (4, tb1), (5, m2), (7, tb2), (8, m3), (9, s2)):
        sent(buf, i)


def per_device(
    nrow, ncol, tile_data, tile_coords, tile_counts, factor_rows, factor_cols, factor_depth, damping
):
    slots, size, _ = tile_data.shape
    rank, wa = factor_rows.shape
    wb, wc = factor_cols.shape[1], factor_depth.shape[1]
    ka, kb = wa // size, wb // size
    ndev = nrow * ncol
    msg = -(-max(wc, slots) // 8) * 8
    vm = pltpu.VMEM
    exchange = [
        vm((ncol, slots, rank, size), F32),
        vm((nrow, slots, rank, size), F32),
        vm((ndev, slots, 128), F32),
    ]

    def line(chunks):
        return [
            pltpu.SemaphoreType.DMA((3, ncol // CORES, chunks)),
            pltpu.SemaphoreType.DMA((ncol, chunks)),
        ]

    vspec = pl.BlockSpec(memory_space=pltpu.VMEM)
    sspec = pl.BlockSpec(memory_space=pltpu.SMEM)
    step_a, step_b, step_c = pl.pallas_call(
        functools.partial(kernel, nrow, ncol),
        out_shape=(
            jax.ShapeDtypeStruct((rank, wa), F32),
            jax.ShapeDtypeStruct((rank, wb), F32),
            jax.ShapeDtypeStruct((wc, rank), F32),
        ),
        in_specs=[vspec, sspec, sspec, sspec, vspec, vspec, vspec],
        out_specs=(vspec, vspec, vspec),
        scratch_shapes=[
            vm((ncol, ka, rank, size), F32),
            vm((nrow, kb, rank, size), F32),
            vm((ndev, msg, 128), F32),
            *exchange,
            *exchange,
            vm((ndev, 4, 128), F32),
            vm((ncol, msg, 128), F32),
            vm((nrow, msg, 128), F32),
            vm((ndev, msg, 128), F32),
            vm((slots + ka, rank, size), F32),
            vm((slots + kb, rank, size), F32),
            vm((slots + ka, rank, size), F32),
            vm((slots + kb, rank, size), F32),
            vm((slots, size, size), F32),
            pltpu.SemaphoreType.DMA((10,)),
            pltpu.SemaphoreType.DMA((10,)),
            *line(ka),
            *line(slots),
            *line(slots),
        ],
        compiler_params=pltpu.CompilerParams(collective_id=0, has_side_effects=True),
    )(
        tile_data, tile_coords, tile_counts, damping.reshape(1),
        factor_rows, factor_cols, factor_depth.T,
    )
    return step_a, step_b, step_c.T


def solution(mesh):
    nrow, ncol = mesh.shape["row"], mesh.shape["col"]
    return jax.shard_map(
        functools.partial(per_device, nrow, ncol),
        mesh=mesh,
        in_specs=(
            P(("row", "col"), None, None),
            P(None, ("row", "col")),
            P(("row", "col")),
            P(None, ("row", "col")),
            P(None, ("col", "row")),
            P(None, ("row", "col")),
            P(),
        ),
        out_specs=(P(None, ("row", "col")), P(None, ("col", "row")), P(None, ("row", "col"))),
        check_vma=False,
    )
```

```python
import functools

import jax
import jax.numpy as jnp
from jax import lax
from jax.experimental import pallas as pl
from jax.experimental.pallas import tpu as pltpu
from jax.sharding import PartitionSpec as P

MESH = pl.DeviceIdType.MESH
CORES = 2
HI = lax.Precision.HIGHEST
F32 = jnp.float32


def dot(x, y, cx, cy):
    return lax.dot_general(
        x, y, (((cx,), (cy,)), ((), ())), precision=HI, preferred_element_type=F32
    )


def total(x):
    return jnp.sum(jnp.sum(x, axis=0, keepdims=True), axis=1, keepdims=True)


def kernel(
    nrow, ncol,
    tile, coords, counts, damp, fa, fb, fc,
    out_a, out_b, out_c,
    ga, gb, m1, ta1, tb1, m2, ta2, tb2, m3, s2,
    pa, pb, pc, da, db, ia, ib, v0,
    gate, send, recv, ls0, lr0, ls1, lr1, ls2, lr2,
):
    slots, size = tile.shape[0], tile.shape[1]
    rank = fa.shape[0]
    wc = fc.shape[0]
    ka, kb = fa.shape[1] // size, fb.shape[1] // size
    ndev = nrow * ncol
    p, q = lax.axis_index("row"), lax.axis_index("col")
    me = p * ncol + q

    def over_all(k):
        d = lax.rem(me + k, ndev)
        return (lax.div(d, ncol), lax.rem(d, ncol))

    def over_col(k):
        return (p, lax.rem(q + k, ncol))

    def over_row(k):
        return (lax.rem(p + k, nrow), q)

    def spread(src, dst, sem, n, where):
        def one(k, _):
            pltpu.make_async_remote_copy(
                src_ref=src, dst_ref=dst, send_sem=send.at[sem], recv_sem=recv.at[sem],
                device_id=where(k), device_id_type=MESH,
            ).start()
            return 0

        lax.fori_loop(1, n, one, 0)

    def arrived(buf, sem):
        part = buf.at[pl.ds(0, buf.shape[0] - 1)]
        pltpu.make_async_copy(part, part, recv.at[sem]).wait()

    def sent(buf, sem):
        part = buf.at[pl.ds(0, buf.shape[0] - 1)]
        pltpu.make_async_copy(part, part, send.at[sem]).wait()

    nz = ncol // CORES
    z, core = lax.div(q, CORES), lax.rem(q, CORES)
    other = CORES - 1 - core

    def move(buf, ls, lr, dz, block, chunk):
        target = (q + CORES, q - CORES, z * CORES + other)[dz]
        piece = buf.at[block * CORES + core, chunk]
        return pltpu.make_async_remote_copy(
            src_ref=piece, dst_ref=piece,
            send_sem=ls.at[dz, block, chunk], recv_sem=lr.at[block * CORES + core, chunk],
            device_id=(p, target), device_id_type=MESH,
        )

    def line_start(buf, ls, lr, chunks):
        for chunk in chunks:
            @pl.when(z + 1 < nz)
            def _():
                move(buf, ls, lr, 0, z, chunk).start()

            @pl.when(z > 0)
            def _():
                move(buf, ls, lr, 1, z, chunk).start()

            move(buf, ls, lr, 2, z, chunk).start()

    def line_relay(buf, ls, lr, use, between):
        chunks = range(buf.shape[1])

        def landed(slot, chunk):
            piece = buf.at[slot, chunk]
            pltpu.make_async_copy(piece, piece, lr.at[slot, chunk]).wait()

        def relay(d):
            for chunk in chunks:
                @pl.when(z - d >= 0)
                def _():
                    block = z - d
                    landed(block * CORES + core, chunk)

                    @pl.when(z + 1 < nz)
                    def _():
                        move(buf, ls, lr, 0, block, chunk).start()

                    move(buf, ls, lr, 2, block, chunk).start()

                @pl.when(z + d < nz)
                def _():
                    block = z + d
                    landed(block * CORES + core, chunk)

                    @pl.when(z > 0)
                    def _():
                        move(buf, ls, lr, 1, block, chunk).start()

                    move(buf, ls, lr, 2, block, chunk).start()

                @pl.when(z - d >= 0)
                def _():
                    use((z - d) * CORES + core, chunk)

                @pl.when(z + d < nz)
                def _():
                    use((z + d) * CORES + core, chunk)

        def partner(d):
            for chunk in chunks:
                @pl.when(z - d >= 0)
                def _():
                    landed((z - d) * CORES + other, chunk)
                    use((z - d) * CORES + other, chunk)

                @pl.when((z + d < nz) & (d > 0))
                def _():
                    landed((z + d) * CORES + other, chunk)
                    use((z + d) * CORES + other, chunk)

        def stage(d, _):
            relay(d)
            partner(d - 1)
            return 0

        for chunk in chunks:
            use(q, chunk)
        lax.fori_loop(1, nz - 1, stage, 0)
        between()
        lax.fori_loop(nz - 1, nz, stage, 0)
        partner(nz - 1)

    def line_sent(buf, ls, lr):
        def one(block, _):
            for chunk in range(buf.shape[1]):
                @pl.when((z + 1 < nz) & (block <= z))
                def _():
                    move(buf, ls, lr, 0, block, chunk).wait_send()

                @pl.when((z > 0) & (block >= z))
                def _():
                    move(buf, ls, lr, 1, block, chunk).wait_send()

                move(buf, ls, lr, 2, block, chunk).wait_send()
            return 0

        lax.fori_loop(0, nz, one, 0)

    barrier = pltpu.get_barrier_semaphore()

    for k in range(1, nrow):
        pl.semaphore_signal(barrier, inc=1, device_id=over_row(k), device_id_type=MESH)
    for k in range(1, ncol):
        pl.semaphore_signal(barrier, inc=1, device_id=over_col(k), device_id_type=MESH)

    row_i = lax.broadcasted_iota(jnp.int32, (rank, 128), 0)
    lane_i = lax.broadcasted_iota(jnp.int32, (rank, 128), 1)
    eye = row_i == lane_i
    msg = m1.shape[1]
    mrow = lax.broadcasted_iota(jnp.int32, (msg, 128), 0)
    mlane = lax.broadcasted_iota(jnp.int32, (msg, 128), 1)
    nrow_i = lax.broadcasted_iota(jnp.int32, (slots, 128), 0)
    nlane = lax.broadcasted_iota(jnp.int32, (slots, 128), 1)

    def as_col(row):
        return jnp.sum(jnp.where(eye, row, 0.0), axis=1, keepdims=True)

    def as_row(col):
        return jnp.sum(jnp.where(eye, col, 0.0), axis=0, keepdims=True)

    first = jnp.where(mlane >= rank, -1.0, jnp.zeros((msg, 128), F32))
    for t in range(slots):
        for c in range(3):
            val = jnp.full((msg, 128), coords[c, t], jnp.int32).astype(F32)
            first = jnp.where((mrow == t) & (mlane == rank + c), val, first)
    m1[me] = first
    m1[me, :wc, :rank] = fc[...]
    for o in range(ka):
        ga[q, o] = fa[:, o * size : (o + 1) * size]
    for o in range(kb):
        gb[p, o] = fb[:, o * size : (o + 1) * size]

    pl.semaphore_wait(barrier, nrow + ncol - 2)
    for k in range(1, nrow):
        pl.semaphore_signal(gate, inc=1, device_id=over_row(k), device_id_type=MESH)
    line_start(ga, ls0, lr0, range(ka))
    spread(gb.at[p], gb.at[p], 1, nrow, over_row)
    pl.semaphore_wait(gate, nrow - 1)
    spread(m1.at[me], m1.at[me], 2, ndev, over_all)

    def place(c, dst):
        def one(s, base):
            blk = m1[base + s]
            dst[s] = jnp.broadcast_to(blk[:, rank + c : rank + c + 1], (msg, 128))
            return base

        return one


    def place_b(s, _):
        blk = m1[s * ncol + q]
        pb[s] = jnp.broadcast_to(blk[:, rank + 1 : rank + 2], (msg, 128))
        return 0

    def place_all():
        arrived(m1, 2)
        lax.fori_loop(0, ncol, place(0, pa), p * ncol)
        lax.fori_loop(0, nrow, place_b, 0)
        lax.fori_loop(0, ndev, place(2, pc), 0)
        arrived(gb, 1)

    line_relay(ga, ls0, lr0, lambda slot, chunk: None, place_all)

    count = counts[0]
    damping = damp[0]

    def splat(val):
        return jnp.full((1, 128), val, jnp.int32).astype(F32)

    my_a = [splat(coords[0, t]) for t in range(slots)]
    my_b = [splat(coords[1, t]) for t in range(slots)]
    my_c = [splat(coords[2, t]) for t in range(slots)]
    own_a = [splat(q * ka + o) for o in range(ka)]
    own_b = [splat(p * kb + o) for o in range(kb)]
    own_c = [splat(me * wc + o) for o in range(wc)]

    def tile_factors(t):
        a, b, k = coords[0, t], coords[1, t], coords[2, t]
        rows_a = ga[lax.div(a, ka), lax.rem(a, ka)]
        rows_b = gb[lax.div(b, kb), lax.rem(b, kb)]
        at = lax.div(k, wc)
        row_c = jnp.sum(jnp.where(mrow + at * wc == k, m1[at], 0.0), axis=0, keepdims=True)
        return rows_a, rows_b, as_col(row_c)

    facs = [tile_factors(t) for t in range(slots)]

    def send_grads(values, ta, tb, m, extra, sem, ls, lr):
        note = extra
        for t in range(slots):
            rows_a, rows_b, col_c = facs[t]
            raw = dot(rows_b, values[t], 1, 1)
            ta[q, t] = raw * col_c
            line_start(ta, ls, lr, (t,))
            tb[p, t] = dot(rows_a * col_c, values[t], 1, 0)
            note = jnp.where(
                (nrow_i == t) & (nlane < rank),
                as_row(jnp.sum(rows_a * raw, axis=1, keepdims=True)), note,
            )
        m[me] = note
        spread(m.at[me], m.at[me], sem + 2, ndev, over_all)
        spread(tb.at[p], tb.at[p], sem + 1, nrow, over_row)

    def live(t, x):
        return jnp.where(jnp.full((size, size), t, jnp.int32) < count, x, 0.0)

    values = [
        live(t, tile[t].astype(F32) - dot(facs[t][0], facs[t][1] * facs[t][2], 0, 0))
        for t in range(slots)
    ]
    send_grads(values, ta1, tb1, m2, jnp.zeros((slots, 128), F32), 3, ls1, lr1)

    def take(acc, buf, tags, wanted):
        def one(slot, chunk):
            g = buf[slot, chunk]
            tag = tags[slot, chunk : chunk + 1, :]
            for i, want in enumerate(wanted):
                acc[i] += g * jnp.where(tag == want, 1.0, 0.0)

        return one

    def collect(ta, tb, m, ls, lr, sem, acc_a, acc_b):
        acc_a[...] = jnp.zeros_like(acc_a)
        acc_b[...] = jnp.zeros_like(acc_b)
        take_b = take(acc_b, tb, pb, my_b + own_b)
        depth = []

        def row_sums(s, _):
            for t in range(slots):
                take_b(s, t)
            return 0

        def between():
            arrived(m, sem + 2)
            depth.extend(depth_sums(m, my_c + own_c))
            arrived(tb, sem + 1)
            lax.fori_loop(0, nrow, row_sums, 0)

        line_relay(ta, ls, lr, take(acc_a, ta, pa, my_a + own_a), between)
        return depth

    def depth_sums(m, wanted):
        def one(s, accs):
            g, tag = m[s], pc[s, :slots]
            return tuple(acc + jnp.where(tag == w, g, 0.0) for acc, w in zip(accs, wanted))

        accs = lax.fori_loop(
            0, ndev, one, tuple(jnp.zeros((slots, 128), F32) for _ in wanted)
        )
        return [
            jnp.sum(jnp.where(nlane < rank, acc, 0.0), axis=0, keepdims=True) for acc in accs
        ]

    depth = collect(ta1, tb1, m2, ls1, lr1, 3, da, db)
    dc, rc = depth[:slots], depth[slots:]

    def inner(xa, xb, xc, ya, yb, yc):
        part = jnp.zeros((rank, size), F32)
        for o in range(ka):
            part += xa(o) * ya(o)
        for o in range(kb):
            part += xb(o) * yb(o)
        res = total(part)
        for o in range(wc):
            res += total(xc[o] * yc[o])
        return res

    get_ra, get_rb = (lambda o: da[slots + o]), (lambda o: db[slots + o])
    norm_part = inner(get_ra, get_rb, rc, get_ra, get_rb, rc)

    def product(t, ua, ub, uc):
        rows_a, rows_b, col_c = facs[t]
        left = jnp.concatenate([ua, rows_a], axis=0)
        right = jnp.concatenate([rows_b * col_c, ub * col_c + rows_b * as_col(uc)], axis=0)
        return live(t, dot(left, right, 0, 0))

    curve = jnp.zeros((size, size), F32)
    values = []
    for t in range(slots):
        v = product(t, da[t], db[t], dc[t])
        v0[t] = v
        curve += v * v
        values.append(v)
    extra = jnp.where(
        nlane == rank, norm_part, jnp.where(nlane == rank + 1, total(curve), 0.0)
    )
    send_grads(values, ta2, tb2, m3, extra, 6, ls2, lr2)

    depth = collect(ta2, tb2, m3, ls2, lr2, 6, ia, ib)
    sums = jnp.sum(m3[...], axis=0)
    norm0 = jnp.broadcast_to(sums[0:1, rank : rank + 1], (1, 128))
    curve0 = jnp.broadcast_to(sums[0:1, rank + 1 : rank + 2], (1, 128))
    alpha0 = norm0 / (curve0 + damping * norm0)

    def next_residual(res, image):
        return res - alpha0 * (image + damping * res)

    for o in range(ka):
        ia[slots + o] = next_residual(da[slots + o], ia[slots + o])
    for o in range(kb):
        ib[slots + o] = next_residual(db[slots + o], ib[slots + o])
    rc1 = [next_residual(rc[o], depth[slots + o]) for o in range(wc)]
    get_a1, get_b1 = (lambda o: ia[slots + o]), (lambda o: ib[slots + o])
    fresh_part = inner(get_a1, get_b1, rc1, get_a1, get_b1, rc1)
    cross_part = inner(get_a1, get_b1, rc1, get_ra, get_rb, rc)
    curve_part = jnp.zeros((size, size), F32)
    mixed_part = jnp.zeros((size, size), F32)
    for t in range(slots):
        v = product(
            t,
            next_residual(da[t], ia[t]),
            next_residual(db[t], ib[t]),
            next_residual(dc[t], depth[t]),
        )
        curve_part += v * v
        mixed_part += v * v0[t]
    parts = (fresh_part, cross_part, total(curve_part), total(mixed_part))
    for i, part in enumerate(parts):
        s2[me, i : i + 1, :] = jnp.broadcast_to(part, (1, 128))
    spread(s2.at[me], s2.at[me], 9, ndev, over_all)
    arrived(s2, 9)
    sums = jnp.sum(s2[...], axis=0)
    fresh, cross, curve_r, mixed = (sums[i : i + 1, :] for i in range(4))
    beta = fresh / norm0
    direct = fresh + beta * (2.0 * cross + beta * norm0)
    curve1 = curve_r + beta * (2.0 * mixed + beta * curve0)
    alpha1 = fresh / (curve1 + damping * direct)

    def step(res, res1):
        return alpha0 * res + alpha1 * (res1 + beta * res)

    for o in range(ka):
        out_a[:, o * size : (o + 1) * size] = step(da[slots + o], ia[slots + o])
    for o in range(kb):
        out_b[:, o * size : (o + 1) * size] = step(db[slots + o], ib[slots + o])
    for o in range(wc):
        out_c[o : o + 1, :] = step(rc[o], rc1[o])[:, :rank]

    line_sent(ga, ls0, lr0)
    line_sent(ta1, ls1, lr1)
    line_sent(ta2, ls2, lr2)
    for i, buf in ((1, gb), (2, m1), (4, tb1), (5, m2), (7, tb2), (8, m3), (9, s2)):
        sent(buf, i)


def per_device(
    nrow, ncol, tile_data, tile_coords, tile_counts, factor_rows, factor_cols, factor_depth, damping
):
    slots, size, _ = tile_data.shape
    rank, wa = factor_rows.shape
    wb, wc = factor_cols.shape[1], factor_depth.shape[1]
    ka, kb = wa // size, wb // size
    ndev = nrow * ncol
    msg = -(-max(wc, slots) // 8) * 8
    vm = pltpu.VMEM
    exchange = [
        vm((ncol, slots, rank, size), F32),
        vm((nrow, slots, rank, size), F32),
        vm((ndev, slots, 128), F32),
    ]

    def line(chunks):
        return [
            pltpu.SemaphoreType.DMA((3, ncol // CORES, chunks)),
            pltpu.SemaphoreType.DMA((ncol, chunks)),
        ]

    vspec = pl.BlockSpec(memory_space=pltpu.VMEM)
    sspec = pl.BlockSpec(memory_space=pltpu.SMEM)
    step_a, step_b, step_c = pl.pallas_call(
        functools.partial(kernel, nrow, ncol),
        out_shape=(
            jax.ShapeDtypeStruct((rank, wa), F32),
            jax.ShapeDtypeStruct((rank, wb), F32),
            jax.ShapeDtypeStruct((wc, rank), F32),
        ),
        in_specs=[vspec, sspec, sspec, sspec, vspec, vspec, vspec],
        out_specs=(vspec, vspec, vspec),
        scratch_shapes=[
            vm((ncol, ka, rank, size), F32),
            vm((nrow, kb, rank, size), F32),
            vm((ndev, msg, 128), F32),
            *exchange,
            *exchange,
            vm((ndev, 4, 128), F32),
            vm((ncol, msg, 128), F32),
            vm((nrow, msg, 128), F32),
            vm((ndev, msg, 128), F32),
            vm((slots + ka, rank, size), F32),
            vm((slots + kb, rank, size), F32),
            vm((slots + ka, rank, size), F32),
            vm((slots + kb, rank, size), F32),
            vm((slots, size, size), F32),
            pltpu.SemaphoreType.REGULAR,
            pltpu.SemaphoreType.DMA((10,)),
            pltpu.SemaphoreType.DMA((10,)),
            *line(ka),
            *line(slots),
            *line(slots),
        ],
        compiler_params=pltpu.CompilerParams(collective_id=0, has_side_effects=True),
    )(
        tile_data, tile_coords, tile_counts, damping.reshape(1),
        factor_rows, factor_cols, factor_depth.T,
    )
    return step_a, step_b, step_c.T


def solution(mesh):
    nrow, ncol = mesh.shape["row"], mesh.shape["col"]
    return jax.shard_map(
        functools.partial(per_device, nrow, ncol),
        mesh=mesh,
        in_specs=(
            P(("row", "col"), None, None),
            P(None, ("row", "col")),
            P(("row", "col")),
            P(None, ("row", "col")),
            P(None, ("col", "row")),
            P(None, ("row", "col")),
            P(),
        ),
        out_specs=(P(None, ("row", "col")), P(None, ("col", "row")), P(None, ("row", "col"))),
        check_vma=False,
    )
```
